256 devices in a mesh: group: 4 (over y, x), blk: 64 (over z, core).
Axes of the slice: x: 2, y: 2, z: 32, core: 2. Of those that a mesh axis runs over, the one named last changes fastest.
The devices are a block of a 4x8x32 slice.
Arguments:
- queries: bfloat16 [8, 256, 2048], P('group', 'blk'), parts along dimension 0, may hold values from -160 to 160
- keys: bfloat16 [8, 81920, 256], P('group', 'blk'), parts along dimension 0, may hold values from -4 to 4
- values: bfloat16 [8, 81920, 256], P('group', 'blk'), parts along dimension 0, may hold values from -6 to 6
- lengths: int32 [8], P('group'), parts along dimension 0, may hold values from 61440 to 81920
- offsets: int32 [8], P('group'), parts along dimension 0, may hold values from 51200 to 81664
Outputs:
- attended: bfloat16 [8, 256, 2048], P('group', 'blk'), parts along dimension 0
The draws below stay inside these ranges and needn't reach their ends.
There are 4 independent parts, one for each index of `group`. The reference program is written for one: setup_inputs(seed, part) draws one part's arguments, and reference() takes and returns one part's arrays. A program takes and returns all parts, laid end to end along the dimension named above; each array names one. Nothing has to cross between parts.
All inputs are finite; a program needn't handle non-finite values.
Results may differ from the reference program's by a relative error of at most 0.0085.
Values may be sent and summed in bfloat16 or wider, within the bound.
A program may use at most 64 MiB of HBM per device.

```python
import math
import jax
import jax.numpy as jnp
from jax import lax

HEADS = 16
KV_HEADS = 2
HEAD_DIM = 128
MICRO = 2
KEYS_DEV = 1280
QUERIES = 256
CONTEXT = 81920
N_BLK = 64


def draw_keys(key, part):
    array_shape = (MICRO, CONTEXT, KV_HEADS * HEAD_DIM)
    sampled = jnp.clip(jax.random.normal(jax.random.fold_in(key, 11), array_shape, jnp.float32), -4.0, 4.0)
    return sampled.astype(jnp.bfloat16)


def draw_queries(key, part):
    array_shape = (MICRO, QUERIES, HEADS * HEAD_DIM)
    sampled = jnp.clip(3.0 * jax.random.normal(jax.random.fold_in(key, 13), array_shape, jnp.float32), -12.0, 12.0)
    return sampled.astype(jnp.bfloat16)


def block_levels(rng, shape, pieces, least, top_value):
    gain, own = 1.0, jax.random.fold_in(rng, 6)
    for dim, shards_of in pieces:
        heights = jnp.exp(jax.random.uniform(jax.random.fold_in(own, dim), (shards_of,), jnp.float32, least / len(pieces), top_value / len(pieces)))
        gain = gain * jnp.repeat(heights, shape[dim] // shards_of).reshape([-1 if axis == dim else 1 for axis in range(len(shape))])
    return gain


def noise(key, dims, spread, most, split=(), kind=jnp.bfloat16):
    factor_of = block_levels(key, dims, split, -0.22, 0.18) if split else 1.0
    drawn = jax.random.normal(key, dims, jnp.float32) * spread * factor_of
    return jnp.minimum(jnp.maximum(drawn, -most), most).astype(kind)


def setup_inputs(seed: int = 0, part: int = 0) -> dict:
    streams_of = jax.random.split(jax.random.key(seed), 6)
    part_splits = jax.random.split(jax.random.fold_in(streams_of[5], part), 6)
    queries = draw_queries(jax.random.fold_in(jax.random.fold_in(streams_of[5], part), 71), part)
    keys = draw_keys(jax.random.fold_in(jax.random.fold_in(streams_of[5], part), 71), part)
    values = noise(part_splits[2], (MICRO, CONTEXT, KV_HEADS * HEAD_DIM), 1.0, 6.0, ((1, 64),))
    lengths = jax.random.randint(part_splits[3], (MICRO,), CONTEXT * 3 // 4, CONTEXT + 1).astype(jnp.int32)
    offsets = jax.random.randint(part_splits[4], (MICRO,), CONTEXT * 5 // 8, CONTEXT - QUERIES + 1).astype(jnp.int32)
    return {"queries": queries, "keys": keys, "values": values, "lengths": lengths, "offsets": offsets}


masked_low = -1e+30

def shard_partial(query_rows, key_rows, value_rows, query_pos, key_pos, lengths):
    micro_count, rows_count, row_width = query_rows.shape
    heads_count = row_width // HEAD_DIM
    group_size = heads_count // KV_HEADS
    query_split = query_rows.astype(jnp.float32).reshape(micro_count, rows_count, KV_HEADS, group_size, HEAD_DIM)
    key_split = key_rows.astype(jnp.float32).reshape(micro_count, key_rows.shape[1], KV_HEADS, HEAD_DIM)
    value_split = value_rows.astype(jnp.float32).reshape(micro_count, value_rows.shape[1], KV_HEADS, HEAD_DIM)
    scores = jnp.einsum('brkgd,bskd->bkgrs', query_split, key_split)
    scores = scores * (1.0 / math.sqrt(HEAD_DIM))
    visible = (key_pos[None, None, :] <= query_pos[:, :, None]) & (key_pos[None, None, :] < lengths[:, None, None])
    visible = visible[:, None, None, :, :]
    any_visible = jnp.any(visible, axis=-1)
    row_max = lax.optimization_barrier(jnp.max(jnp.where(visible, scores, masked_low), axis=-1))
    safe_max = jnp.where(any_visible, row_max, 0.0)
    shifted = jnp.where(visible, scores - safe_max[..., None], 0.0)
    weights = jnp.where(visible, jnp.exp(shifted), 0.0)
    totals = lax.optimization_barrier(jnp.sum(weights, axis=-1))
    bounded = jnp.maximum(totals, 1.0)
    rounded = lax.optimization_barrier(weights.astype(jnp.bfloat16)).astype(jnp.float32)
    numerator = jnp.einsum('bkgrs,bskd->bkgrd', rounded, value_split)
    partial_value = (numerator / bounded[..., None]).astype(jnp.bfloat16)
    partial_value = jnp.transpose(partial_value, (0, 3, 1, 2, 4)).reshape(micro_count, rows_count, row_width)
    logsum = jnp.where(any_visible, safe_max + jnp.log(bounded), masked_low)
    logsum = jnp.transpose(logsum, (0, 3, 1, 2)).reshape(micro_count, rows_count, heads_count)
    return (partial_value, logsum)

def reference(queries, keys, values, lengths, offsets):
    micro_count, all_rows, row_width = queries.shape
    heads_count = row_width // HEAD_DIM
    query_pos = offsets[:, None] + jnp.arange(all_rows, dtype=jnp.int32)[None, :]

    def visit(state, shard_index):
        best_log, scale_total, accumulated = state
        start_key = (shard_index * KEYS_DEV).astype(jnp.int32)
        key_rows = lax.dynamic_slice_in_dim(keys, start_key, KEYS_DEV, 1)
        value_rows = lax.dynamic_slice_in_dim(values, start_key, KEYS_DEV, 1)
        key_pos = start_key + jnp.arange(KEYS_DEV, dtype=jnp.int32)
        partial_value, logsum = shard_partial(queries, key_rows, value_rows, query_pos, key_pos, lengths)
        partial_value = lax.optimization_barrier(partial_value).astype(jnp.float32)
        partial_value = partial_value.reshape(micro_count, all_rows, heads_count, HEAD_DIM)
        newest = jnp.maximum(best_log, logsum)
        keep_old = jnp.exp(best_log - newest)
        take_new = jnp.exp(logsum - newest)
        new_total = scale_total * keep_old + take_new
        new_accum = accumulated * keep_old[..., None] + partial_value * take_new[..., None]
        return ((newest, new_total, new_accum), None)
    initial = (jnp.full((micro_count, all_rows, heads_count), masked_low, jnp.float32), jnp.zeros((micro_count, all_rows, heads_count), jnp.float32), jnp.zeros((micro_count, all_rows, heads_count, HEAD_DIM), jnp.float32))
    final_state, unused = lax.scan(visit, initial, jnp.arange(N_BLK, dtype=jnp.int32))
    best_log, scale_total, accumulated = final_state
    merged = accumulated / scale_total[..., None]
    return merged.reshape(micro_count, all_rows, row_width).astype(jnp.bfloat16)
```

```python
import functools
import math

import jax
import jax.numpy as jnp
from jax import lax
from jax.experimental import pallas as pl
from jax.experimental.pallas import tpu as pltpu
from jax.sharding import PartitionSpec as P

KV_HEADS = 2
HEAD_DIM = 128
CORES = 2
MESH = pl.DeviceIdType.MESH
EXP_SCALE = math.log2(math.e) / math.sqrt(HEAD_DIM)
LOW = -1e30
TILE = 256


def step_of(distance, strides):
    for stride in strides:
        if distance % stride == 0:
            return stride
    return 1


def merge(parts):
    best = functools.reduce(jnp.maximum, [part[1] for part in parts])
    scales = [jnp.exp2((part[1] - best) * EXP_SCALE) for part in parts]
    numer = sum(part[0].astype(jnp.float32) * scale for part, scale in zip(parts, scales))
    total = sum(part[2] * scale for part, scale in zip(parts, scales))
    return numer, best, total


def attend(keys, values_t, rows, limit):
    width = rows.shape[0]
    position = lax.broadcasted_iota(jnp.int32, (TILE, width), 0)
    best = numer = total = None
    for tile in range(keys.shape[0] // TILE):
        here = slice(tile * TILE, (tile + 1) * TILE)
        scores = lax.dot_general(
            keys[here, :], rows, (((1,), (1,)), ((), ())), preferred_element_type=jnp.float32
        )
        scores = jnp.where(position < limit - tile * TILE, scores, LOW)
        largest = scores.reshape(TILE // 8, 8, width).max(0).max(0, keepdims=True)
        newest = largest if best is None else jnp.maximum(best, largest)
        weights = jnp.exp2((scores - newest) * EXP_SCALE)
        sums = weights.reshape(TILE // 8, 8, width).sum(0)
        product = jnp.dot(
            values_t[:, here], weights.astype(jnp.bfloat16), preferred_element_type=jnp.float32
        )
        if best is None:
            numer, total = product, sums
        else:
            keep = jnp.exp2((best - newest) * EXP_SCALE)
            numer, total = numer * keep + product, total * keep + sums
        best = newest
    return numer, best, total.sum(0, keepdims=True)


def kernel(
    chips,
    heads,
    strides,
    lengths,
    offsets,
    q_in,
    k_in,
    v_in,
    out,
    keys,
    values,
    values_t,
    pick,
    q_all,
    part,
    stat,
    send,
    got,
    got_stat,
    home,
    home_got,
    local_sem,
    pair_send,
    pair_recv,
    q_send,
    q_recv,
    o_send,
    o_recv,
    s_send,
    s_recv,
):
    half = chips // 2
    group = lax.axis_index("group")
    me = lax.axis_index("blk")
    core = lax.rem(me, CORES)
    other = 1 - core
    chip = lax.div(me, CORES)
    shard = k_in.shape[1]
    rows_half = q_in.shape[1]
    columns = CORES * rows_half

    def device(z, on):
        return (group, lax.rem(z + chips, chips) * CORES + on)

    partner = device(chip, other)

    barrier = pltpu.get_barrier_semaphore()
    pl.semaphore_signal(barrier, inc=1, device_id=partner, device_id_type=MESH)
    for stride in strides:
        for way in (-1, 1):
            pl.semaphore_signal(
                barrier, inc=1, device_id=device(chip + way * stride, core), device_id_type=MESH
            )
    my_rows = pl.ds(pl.multiple_of(core * shard, 256), shard)
    my_half = pl.ds(pl.multiple_of(core * rows_half, 64), rows_half)
    locals_ = [
        pltpu.make_async_copy(q_in.at[core], q_all.at[0, 0, my_half], local_sem.at[0]),
        pltpu.make_async_copy(v_in.at[core], values.at[my_rows], local_sem.at[1]),
        pltpu.make_async_copy(k_in.at[core], keys.at[my_rows], local_sem.at[2]),
    ]
    for copy in locals_:
        copy.start()
    pl.semaphore_wait(barrier, 1 + 2 * len(strides))

    def to_partner(src, dst, index):
        return pltpu.make_async_remote_copy(
            src_ref=src,
            dst_ref=dst,
            send_sem=pair_send.at[index],
            recv_sem=pair_recv.at[index],
            device_id=partner,
            device_id_type=MESH,
        )

    swaps = [
        to_partner(q_in.at[other], q_all.at[0, 0, my_half], 0),
        to_partner(v_in.at[other], values.at[my_rows], 1),
        to_partner(k_in.at[other], keys.at[my_rows], 2),
    ]
    for copy in swaps:
        copy.start()

    row = lax.broadcasted_iota(jnp.int32, (columns, HEAD_DIM), 0)
    low = (lax.rem(row, heads) < heads // KV_HEADS).astype(jnp.float32)
    pick[0] = low.astype(jnp.bfloat16)
    pick[1] = (1.0 - low).astype(jnp.bfloat16)

    def relay(way, k, stride, src):
        slot = k + stride
        return pltpu.make_async_remote_copy(
            src_ref=src,
            dst_ref=q_all.at[way, slot],
            send_sem=q_send.at[way, slot],
            recv_sem=q_recv.at[way, slot],
            device_id=device(chip + (1 - 2 * way) * stride, core),
            device_id_type=MESH,
        )

    def arrival(way, k):
        return pltpu.make_async_remote_copy(
            src_ref=q_all.at[way, k],
            dst_ref=q_all.at[way, k],
            send_sem=q_send.at[way, k],
            recv_sem=q_recv.at[way, k],
            device_id=partner,
            device_id_type=MESH,
        )

    locals_[0].wait()
    swaps[0].wait()
    for stride in strides:
        for way in (0, 1):
            relay(way, 0, stride, q_all.at[0, 0]).start()
    q_all[1, half] = q_all[0, 0]

    locals_[1].wait()
    swaps[1].wait()
    for tile in range(values.shape[0] // TILE):
        here = slice(tile * TILE, (tile + 1) * TILE)
        values_t[:, here] = values[here, :].T
    locals_[2].wait()
    swaps[2].wait()

    length = lengths[core]
    offset = offsets[core]
    base = chip * CORES * shard
    column = lax.broadcasted_iota(jnp.int32, (1, columns), 1)
    head_low = lax.rem(column, heads) < heads // KV_HEADS

    def limit_of(source):
        position = offset + source * (columns // heads) + lax.div(column, heads)
        return jnp.minimum(position + 1, length) - base

    def homeward(way, k, stride):
        target = device(chip - (1 - 2 * way) * stride, core)
        return [
            pltpu.make_async_remote_copy(
                src_ref=stat.at[way, k],
                dst_ref=got_stat.at[way, k],
                send_sem=s_send.at[way, k],
                recv_sem=s_recv.at[way, k],
                device_id=target,
                device_id_type=MESH,
            ),
            pltpu.make_async_remote_copy(
                src_ref=send.at[way, k],
                dst_ref=got.at[way, k],
                send_sem=o_send.at[way, k],
                recv_sem=o_recv.at[way, k],
                device_id=target,
                device_id_type=MESH,
            ),
        ]

    def visit(k, unused):
        arrival(0, k).wait_recv()

        @pl.when(k < half)
        def _():
            arrival(1, k).wait_recv()

        for place, stride in enumerate(strides):
            turn = lax.rem(k, strides[max(place - 1, 0)]) == 0

            @pl.when(turn & (k + stride <= half))
            def _(stride=stride):
                relay(0, k, stride, q_all.at[0, k]).start()

            @pl.when(turn & (k + stride < half))
            def _(stride=stride):
                relay(1, k, stride, q_all.at[1, k]).start()

        rows = jnp.concatenate([q_all[0, k], q_all[1, k]], axis=0)
        mask = jnp.concatenate([pick[...], pick[...]], axis=1)
        rows = jnp.concatenate([rows * mask[0], rows * mask[1]], axis=1)
        back = lax.select(k == half, 0, k)
        limit = jnp.concatenate(
            [
                limit_of(lax.rem(chip - k + chips, chips)),
                limit_of(lax.rem(chip + back, chips)),
            ],
            axis=1,
        )
        numer, best, total = attend(keys, values_t, rows, limit)
        for way in (0, 1):
            here = slice(way * columns, (way + 1) * columns)
            mine = jnp.where(head_low, numer[:HEAD_DIM, here], numer[HEAD_DIM:, here])
            part[way, k] = mine
            send[way, k] = mine.astype(jnp.bfloat16)
            stat[way, k, 0:1] = best[:, here]
            stat[way, k, 1:2] = total[:, here]

        @pl.when(lax.rem(k, 2) == 1)
        def _():
            for way in (0, 1):
                for copy in homeward(way, k, 1):
                    copy.start()

        return unused

    lax.fori_loop(1, half + 1, visit, 0)
    for copy in homeward(0, half, strides[0]):
        copy.start()

    def own(way, k):
        return part[way, k], stat[way, k, 0:1], stat[way, k, 1:2]

    def received(way, k):
        for copy in homeward(way, k, 1):
            copy.wait_recv()
        return got[way, k], got_stat[way, k, 0:1], got_stat[way, k, 1:2]

    order = sorted(range(2, half, 2), key=lambda k: (step_of(k, strides), -k))
    for k in order:
        stride = step_of(k, strides)
        for way in (0, 1):
            children = [
                k + s
                for s in strides
                if s <= stride
                and k + s <= half - way
                and step_of(k + s, strides) == s
                and (s < stride or stride == strides[0])
            ]
            children.sort(key=lambda child: child - k)
            state = merge([own(way, k)] + [received(way, c) for c in children if c - k < strides[0]])
            for child in children:
                if child - k == strides[0]:
                    state = merge([state, received(way, child)])
            send[way, k] = state[0].astype(jnp.bfloat16)
            stat[way, k, 0:1] = state[1]
            stat[way, k, 1:2] = state[2]
            for copy in homeward(way, k, stride):
                copy.start()

    state = merge(
        [own(1, half)] + [received(way, s) for s in reversed(strides[1:]) for way in (0, 1)]
    )
    state = merge([state] + [received(way, strides[0]) for way in (0, 1)])
    merged = (state[0] / state[2]).T
    home[...] = merged.astype(jnp.bfloat16)
    their_half = pl.ds(pl.multiple_of(other * rows_half, 64), rows_half)
    back = to_partner(home.at[their_half], home_got, 3)
    back.start()
    out[core] = home[my_half]
    back.wait()
    out[other] = home_got[...]

    for way in (0, 1):
        for k in range(1, half + 1 - way):
            arrival(way, k).wait_send()
            for copy in homeward(way, k, 1):
                copy.wait_send()


def body(queries, keys, values, lengths, offsets):
    micro, local_rows, row_width = queries.shape
    shard, kv_width = keys.shape[1:]
    heads = row_width // HEAD_DIM
    chips = lax.axis_size("blk") // CORES
    half = chips // 2
    strides = (4, 2, 1)
    rows_half = local_rows * heads
    columns = CORES * rows_half
    packed = queries.reshape(micro, rows_half, HEAD_DIM)
    slots = (2, half + 1)
    dma = pltpu.SemaphoreType.DMA
    out = pl.pallas_call(
        functools.partial(kernel, chips, heads, strides),
        out_shape=jax.ShapeDtypeStruct((micro, rows_half, HEAD_DIM), jnp.bfloat16),
        in_specs=[
            pl.BlockSpec(memory_space=pltpu.SMEM),
            pl.BlockSpec(memory_space=pltpu.SMEM),
            pl.BlockSpec(memory_space=pl.ANY),
            pl.BlockSpec(memory_space=pl.ANY),
            pl.BlockSpec(memory_space=pl.ANY),
        ],
        out_specs=pl.BlockSpec(memory_space=pltpu.VMEM),
        scratch_shapes=[
            pltpu.VMEM((CORES * shard, kv_width), jnp.bfloat16),
            pltpu.VMEM((CORES * shard, kv_width), jnp.bfloat16),
            pltpu.VMEM((kv_width, CORES * shard), jnp.bfloat16),
            pltpu.VMEM((2, columns, HEAD_DIM), jnp.bfloat16),
            pltpu.VMEM(slots + (columns, HEAD_DIM), jnp.bfloat16),
            pltpu.VMEM(slots + (HEAD_DIM, columns), jnp.float32),
            pltpu.VMEM(slots + (8, columns), jnp.float32),
            pltpu.VMEM(slots + (HEAD_DIM, columns), jnp.bfloat16),
            pltpu.VMEM(slots + (HEAD_DIM, columns), jnp.bfloat16),
            pltpu.VMEM(slots + (8, columns), jnp.float32),
            pltpu.VMEM((columns, HEAD_DIM), jnp.bfloat16),
            pltpu.VMEM((rows_half, HEAD_DIM), jnp.bfloat16),
            dma((3,)),
            dma((4,)),
            dma((4,)),
            dma(slots),
            dma(slots),
            dma(slots),
            dma(slots),
            dma(slots),
            dma(slots),
        ],
        compiler_params=pltpu.CompilerParams(
            collective_id=0, has_side_effects=True, vmem_limit_bytes=48 * 2**20
        ),
        name="attend_all",
    )(lengths, offsets, packed, keys, values)
    return out.reshape(micro, local_rows, row_width)


def solution(mesh):
    return jax.shard_map(
        body,
        mesh=mesh,
        in_specs=(
            P("group", "blk", None),
            P("group", "blk", None),
            P("group", "blk", None),
            P("group"),
            P("group"),
        ),
        out_specs=P("group", "blk", None),
        check_vma=False,
    )
```

```python
import functools
import math

import jax
import jax.numpy as jnp
from jax import lax
from jax.experimental import pallas as pl
from jax.experimental.pallas import tpu as pltpu
from jax.sharding import PartitionSpec as P

KV_HEADS = 2
HEAD_DIM = 128
CORES = 2
MESH = pl.DeviceIdType.MESH
EXP_SCALE = math.log2(math.e) / math.sqrt(HEAD_DIM)
LOW = -1e30
TILE = 256
PIECES = 1


def step_of(distance, strides):
    return next(stride for stride in strides if distance % stride == 0)


def fed_by(distance, furthest, strides):
    return [
        distance + stride
        for stride in strides
        if distance + stride <= furthest and step_of(distance + stride, strides) == stride
    ]


def merge(parts):
    best = functools.reduce(jnp.maximum, [part[1] for part in parts])
    scales = [jnp.exp2((part[1] - best) * EXP_SCALE) for part in parts]
    numer = sum(part[0].astype(jnp.float32) * scale for part, scale in zip(parts, scales))
    total = sum(part[2] * scale for part, scale in zip(parts, scales))
    return numer, best, total


def attend(keys, values_t, scores_ref, rows, limit, last_best):
    width = rows.shape[0]
    position = lax.broadcasted_iota(jnp.int32, (TILE, width), 0)
    columns = rows.astype(jnp.float32).T.astype(jnp.bfloat16)
    best = numer = total = None
    for tile in range(keys.shape[0] // TILE):
        here = slice(tile * TILE, (tile + 1) * TILE)
        last = scores_ref[here, :]
        scores = jnp.dot(keys[here, :], columns, preferred_element_type=jnp.float32)
        scores = jnp.where(position < limit - tile * TILE, scores, LOW)
        largest = scores.reshape(TILE // 8, 8, width).max(0)
        best = largest if best is None else jnp.maximum(best, largest)
        weights = jnp.exp2((last - last_best) * EXP_SCALE)
        scores_ref[here, :] = scores
        sums = weights.reshape(TILE // 8, 8, width).sum(0)
        total = sums if total is None else total + sums
        product = jnp.dot(
            values_t[:, here], weights.astype(jnp.bfloat16), preferred_element_type=jnp.float32
        )
        numer = product if numer is None else numer + product
    return best.max(0, keepdims=True), numer, total.sum(0, keepdims=True)


def kernel(
    chips,
    heads,
    gather_strides,
    home_strides,
    lengths,
    offsets,
    q_in,
    k_in,
    v_in,
    out,
    keys,
    values,
    values_t,
    scores,
    pick,
    q_all,
    part,
    stat,
    send,
    got,
    got_stat,
    home,
    home_got,
    local_sem,
    pair_send,
    pair_recv,
    q_send,
    q_recv,
    o_send,
    o_recv,
    s_send,
    s_recv,
):
    half = chips // 2
    group = lax.axis_index("group")
    me = lax.axis_index("blk")
    core = lax.rem(me, CORES)
    other = 1 - core
    chip = lax.div(me, CORES)
    shard = k_in.shape[1]
    rows_half = q_in.shape[1]
    columns = CORES * rows_half

    def device(z, on):
        return (group, lax.rem(z + chips, chips) * CORES + on)

    partner = device(chip, other)

    barrier = pltpu.get_barrier_semaphore()
    pl.semaphore_signal(barrier, inc=1, device_id=partner, device_id_type=MESH)
    peers = sorted(set(gather_strides + home_strides))
    for stride in peers:
        for way in (-1, 1):
            pl.semaphore_signal(
                barrier, inc=1, device_id=device(chip + way * stride, core), device_id_type=MESH
            )
    my_rows = pl.ds(pl.multiple_of(core * shard, 256), shard)
    my_half = pl.ds(pl.multiple_of(core * rows_half, 64), rows_half)
    locals_ = [
        pltpu.make_async_copy(q_in.at[core], q_all.at[0, 0, my_half], local_sem.at[0]),
        pltpu.make_async_copy(v_in.at[core], values.at[my_rows], local_sem.at[1]),
        pltpu.make_async_copy(k_in.at[core], keys.at[my_rows], local_sem.at[2]),
    ]
    for copy in locals_:
        copy.start()
    pl.semaphore_wait(barrier, 1 + 2 * len(peers))

    def to_partner(src, dst, index):
        return pltpu.make_async_remote_copy(
            src_ref=src,
            dst_ref=dst,
            send_sem=pair_send.at[index],
            recv_sem=pair_recv.at[index],
            device_id=partner,
            device_id_type=MESH,
        )

    swaps = [
        to_partner(q_in.at[other], q_all.at[0, 0, my_half], 0),
        to_partner(v_in.at[other], values.at[my_rows], 1),
        to_partner(k_in.at[other], keys.at[my_rows], 2),
    ]
    for copy in swaps:
        copy.start()

    row = lax.broadcasted_iota(jnp.int32, (columns, HEAD_DIM), 0)
    low = (lax.rem(row, heads) < heads // KV_HEADS).astype(jnp.float32)
    pick[0] = low.astype(jnp.bfloat16)
    pick[1] = (1.0 - low).astype(jnp.bfloat16)

    def relay(way, k, slot, src):
        return pltpu.make_async_remote_copy(
            src_ref=src,
            dst_ref=q_all.at[way, slot],
            send_sem=q_send.at[way, slot],
            recv_sem=q_recv.at[way, slot],
            device_id=device(chip + (1 - 2 * way) * (slot - k), core),
            device_id_type=MESH,
        )

    def arrival(way, k):
        return pltpu.make_async_remote_copy(
            src_ref=q_all.at[way, k],
            dst_ref=q_all.at[way, k],
            send_sem=q_send.at[way, k],
            recv_sem=q_recv.at[way, k],
            device_id=partner,
            device_id_type=MESH,
        )

    locals_[0].wait()
    swaps[0].wait()
    for slot in fed_by(0, half, gather_strides):
        for way in (0, 1):
            relay(way, 0, slot, q_all.at[0, 0]).start()
    q_all[1, half] = q_all[0, 0]

    locals_[1].wait()
    swaps[1].wait()
    for tile in range(values.shape[0] // TILE):
        here = slice(tile * TILE, (tile + 1) * TILE)
        values_t[:, here] = values[here, :].T
    locals_[2].wait()
    swaps[2].wait()

    length = lengths[core]
    offset = offsets[core]
    base = chip * CORES * shard
    column = lax.broadcasted_iota(jnp.int32, (1, columns), 1)
    head_low = lax.rem(column, heads) < heads // KV_HEADS

    def limit_of(source):
        position = offset + source * (columns // heads) + lax.div(column, heads)
        return jnp.minimum(position + 1, length) - base

    def pieces(k):
        return PIECES if k % home_strides[0] == 0 else 1

    def homeward(way, k, stride, count):
        target = device(chip - (1 - 2 * way) * stride, core)
        copies = [
            pltpu.make_async_remote_copy(
                src_ref=stat.at[way, k],
                dst_ref=got_stat.at[way, k],
                send_sem=s_send.at[way, k],
                recv_sem=s_recv.at[way, k],
                device_id=target,
                device_id_type=MESH,
            )
        ]
        size = HEAD_DIM // count
        for piece in range(count):
            span = pl.ds(piece * size, size)
            copies.append(
                pltpu.make_async_remote_copy(
                    src_ref=send.at[way, k, span],
                    dst_ref=got.at[way, k, span],
                    send_sem=o_send.at[way, k, piece],
                    recv_sem=o_recv.at[way, k, piece],
                    device_id=target,
                    device_id_type=MESH,
                )
            )
        return copies

    def own(way, k):
        return part[way, k], stat[way, k, 0:1], stat[way, k, 1:2]

    def received(way, k):
        for copy in homeward(way, k, 1, pieces(k)):
            copy.wait_recv()
        return got[way, k], got_stat[way, k, 0:1], got_stat[way, k, 1:2]

    def keep(way, k, state):
        part[way, k] = state[0]
        stat[way, k, 0:1] = state[1]
        stat[way, k, 1:2] = state[2]

    def gather(way, k):
        nearby = [c for c in fed_by(k, half - way, home_strides) if c - k < home_strides[0]]
        keep(way, k, merge([own(way, k)] + [received(way, c) for c in nearby]))

    def forward(way, k):
        stride = step_of(k, home_strides)
        far = k + home_strides[0]
        copies = homeward(way, k, stride, pieces(k))
        if stride == home_strides[0] and far <= half - way:
            coming = homeward(way, far, 1, PIECES)
            coming[0].wait_recv()
            best = jnp.maximum(stat[way, k, 0:1], got_stat[way, far, 0:1])
            mine = jnp.exp2((stat[way, k, 0:1] - best) * EXP_SCALE)
            theirs = jnp.exp2((got_stat[way, far, 0:1] - best) * EXP_SCALE)
            stat[way, k, 0:1] = best
            stat[way, k, 1:2] = stat[way, k, 1:2] * mine + got_stat[way, far, 1:2] * theirs
            size = HEAD_DIM // PIECES
            for piece in range(PIECES):
                span = slice(piece * size, (piece + 1) * size)
                coming[1 + piece].wait_recv()
                joined = part[way, k, span] * mine + got[way, far, span] * theirs
                send[way, k, span] = joined.astype(jnp.bfloat16)
                if piece == 0:
                    copies[0].start()
                copies[1 + piece].start()
        else:
            send[way, k] = part[way, k].astype(jnp.bfloat16)
            for copy in copies:
                copy.start()

    def ways(k):
        return [way for way in (0, 1) if k <= half - way]

    def await_block(way, k):
        arrival(way, k).wait_recv()

    top = gather_strides[0]
    near = half - top

    def chunk_at(turn):
        return jnp.where(turn < near, turn + 1, half + near - turn)

    scores[...] = jnp.zeros(scores.shape, scores.dtype)

    def visit(turn, last_best):
        for start in range(0, half, top):

            @pl.when(turn == start)
            def _(start=start):
                k = start + top
                for way in ways(k):
                    await_block(way, k)
                    if k + top <= half - way:
                        relay(way, k, k + top, q_all.at[way, k]).start()
                for slot in fed_by(k, half, gather_strides)[1:]:
                    for way in ways(slot):
                        relay(way, k, slot, q_all.at[way, k]).start()
                for way in (0, 1):
                    await_block(way, start + 2)
                    relay(way, start + 2, start + 3, q_all.at[way, start + 2]).start()
                for way in (0, 1):
                    await_block(way, start + 1)

            @pl.when(turn == (start + 1 if start == near else start + 2))
            def _(start=start):
                for way in (0, 1):
                    await_block(way, start + 3)

        k = chunk_at(jnp.minimum(turn, half - 1))
        rows = jnp.concatenate([q_all[0, k], q_all[1, k]], axis=0)
        mask = jnp.concatenate([pick[...], pick[...]], axis=1)
        rows = jnp.concatenate([rows * mask[0], rows * mask[1]], axis=1)
        back = lax.select(k == half, 0, k)
        limit = jnp.concatenate(
            [
                limit_of(lax.rem(chip - k + chips, chips)),
                limit_of(lax.rem(chip + back, chips)),
            ],
            axis=1,
        )
        best, numer, total = attend(keys, values_t, scores, rows, limit, last_best)
        done = chunk_at(jnp.maximum(turn - 1, 0))
        for way in (0, 1):
            here = slice(way * columns, (way + 1) * columns)
            mine = jnp.where(head_low, numer[:HEAD_DIM, here], numer[HEAD_DIM:, here])
            keep(way, done, (mine, last_best[:, here], total[:, here]))
            send[way, done] = mine.astype(jnp.bfloat16)

        @pl.when((lax.rem(done, 2) == 1) & (turn > 0))
        def _():
            for way in (0, 1):
                for copy in homeward(way, done, 1, 1):
                    copy.start()

        @pl.when(turn == near + 1)
        def _():
            forward(0, half)

        for start in range(0, near, top):

            @pl.when(turn == start + top + 2)
            def _(start=start):
                for way in (0, 1):
                    gather(way, start + 2)
                    forward(way, start + 2)

        return best

    lax.fori_loop(0, half + 1, visit, jnp.zeros((1, 2 * columns), jnp.float32))

    for way in (0, 1):
        gather(way, near + 2)
        forward(way, near + 2)
    order = sorted(range(top, half, top), key=lambda k: (step_of(k, home_strides), -k))
    for k in order:
        for way in (0, 1):
            gather(way, k)
            forward(way, k)
    state = merge(
        [own(1, half)]
        + [
            received(way, s)
            for s in fed_by(0, half, home_strides)
            if s < home_strides[0]
            for way in (0, 1)
        ]
    )
    state = merge([state] + [received(way, home_strides[0]) for way in (0, 1)])
    merged = (state[0] / state[2]).T
    home[...] = merged.astype(jnp.bfloat16)
    their_half = pl.ds(pl.multiple_of(other * rows_half, 64), rows_half)
    back = to_partner(home.at[their_half], home_got, 3)
    back.start()
    out[core] = home[my_half]
    back.wait()
    out[other] = home_got[...]

    for way in (0, 1):
        for k in range(1, half + 1 - way):
            arrival(way, k).wait_send()
            for copy in homeward(way, k, 1, pieces(k)):
                copy.wait_send()


def body(queries, keys, values, lengths, offsets):
    micro, local_rows, row_width = queries.shape
    shard, kv_width = keys.shape[1:]
    heads = row_width // HEAD_DIM
    chips = lax.axis_size("blk") // CORES
    half = chips // 2
    rows_half = local_rows * heads
    columns = CORES * rows_half
    packed = queries.reshape(micro, rows_half, HEAD_DIM)
    slots = (2, half + 1)
    dma = pltpu.SemaphoreType.DMA
    out = pl.pallas_call(
        functools.partial(kernel, chips, heads, (4, 2, 1), (4, 2, 1)),
        out_shape=jax.ShapeDtypeStruct((micro, rows_half, HEAD_DIM), jnp.bfloat16),
        in_specs=[
            pl.BlockSpec(memory_space=pltpu.SMEM),
            pl.BlockSpec(memory_space=pltpu.SMEM),
            pl.BlockSpec(memory_space=pl.ANY),
            pl.BlockSpec(memory_space=pl.ANY),
            pl.BlockSpec(memory_space=pl.ANY),
        ],
        out_specs=pl.BlockSpec(memory_space=pltpu.VMEM),
        scratch_shapes=[
            pltpu.VMEM((CORES * shard, kv_width), jnp.bfloat16),
            pltpu.VMEM((CORES * shard, kv_width), jnp.bfloat16),
            pltpu.VMEM((kv_width, CORES * shard), jnp.bfloat16),
            pltpu.VMEM((CORES * shard, 2 * columns), jnp.float32),
            pltpu.VMEM((2, columns, HEAD_DIM), jnp.bfloat16),
            pltpu.VMEM(slots + (columns, HEAD_DIM), jnp.bfloat16),
            pltpu.VMEM(slots + (HEAD_DIM, columns), jnp.float32),
            pltpu.VMEM(slots + (8, columns), jnp.float32),
            pltpu.VMEM(slots + (HEAD_DIM, columns), jnp.bfloat16),
            pltpu.VMEM(slots + (HEAD_DIM, columns), jnp.bfloat16),
            pltpu.VMEM(slots + (8, columns), jnp.float32),
            pltpu.VMEM((columns, HEAD_DIM), jnp.bfloat16),
            pltpu.VMEM((rows_half, HEAD_DIM), jnp.bfloat16),
            dma((3,)),
            dma((4,)),
            dma((4,)),
            dma(slots),
            dma(slots),
            dma(slots + (PIECES,)),
            dma(slots + (PIECES,)),
            dma(slots),
            dma(slots),
        ],
        compiler_params=pltpu.CompilerParams(
            collective_id=0, has_side_effects=True, vmem_limit_bytes=48 * 2**20
        ),
        name="attend_all",
    )(lengths, offsets, packed, keys, values)
    return out.reshape(micro, local_rows, row_width)


def solution(mesh):
    return jax.shard_map(
        body,
        mesh=mesh,
        in_specs=(
            P("group", "blk", None),
            P("group", "blk", None),
            P("group", "blk", None),
            P("group"),
            P("group"),
        ),
        out_specs=P("group", "blk", None),
        check_vma=False,
    )
```

```python
import functools
import math

import jax
import jax.numpy as jnp
from jax import lax
from jax.experimental import pallas as pl
from jax.experimental.pallas import tpu as pltpu
from jax.sharding import PartitionSpec as P

KV_HEADS = 2
HEAD_DIM = 128
CORES = 2
MESH = pl.DeviceIdType.MESH
EXP_SCALE = math.log2(math.e) / math.sqrt(HEAD_DIM)
LOW = -1e30
TILE = 256
PIECES = 1


def step_of(distance, strides):
    return next(stride for stride in strides if distance % stride == 0)


def fed_by(distance, furthest, strides):
    return [
        distance + stride
        for stride in strides
        if distance + stride <= furthest and step_of(distance + stride, strides) == stride
    ]


def merge(parts):
    best = functools.reduce(jnp.maximum, [part[1] for part in parts])
    scales = [jnp.exp2((part[1] - best) * EXP_SCALE) for part in parts]
    numer = sum(part[0].astype(jnp.float32) * scale for part, scale in zip(parts, scales))
    total = sum(part[2] * scale for part, scale in zip(parts, scales))
    return numer, best, total


def attend(keys, values_t, scores_ref, rows, limit, last_best):
    width = rows.shape[0]
    position = lax.broadcasted_iota(jnp.int32, (TILE, width), 0)
    columns = rows.astype(jnp.float32).T.astype(jnp.bfloat16)
    best = numer = total = None
    for tile in range(keys.shape[0] // TILE):
        here = slice(tile * TILE, (tile + 1) * TILE)
        last = scores_ref[here, :]
        scores = jnp.dot(keys[here, :], columns, preferred_element_type=jnp.float32)
        scores = jnp.where(position < limit - tile * TILE, scores, LOW)
        largest = scores.reshape(TILE // 8, 8, width).max(0)
        best = largest if best is None else jnp.maximum(best, largest)
        weights = jnp.exp2((last - last_best) * EXP_SCALE)
        scores_ref[here, :] = scores
        sums = weights.reshape(TILE // 8, 8, width).sum(0)
        total = sums if total is None else total + sums
        product = jnp.dot(
            values_t[:, here], weights.astype(jnp.bfloat16), preferred_element_type=jnp.float32
        )
        numer = product if numer is None else numer + product
    return best.max(0, keepdims=True), numer, total.sum(0, keepdims=True)


def kernel(
    chips,
    heads,
    gather_strides,
    home_strides,
    lengths,
    offsets,
    q_in,
    k_in,
    v_in,
    out,
    keys,
    values,
    values_t,
    scores,
    pick,
    k_stage,
    v_stage,
    q_raw,
    wide,
    packed,
    q_all,
    part,
    stat,
    send,
    got,
    got_stat,
    home,
    home_got,
    local_sem,
    pair_send,
    pair_recv,
    first_send,
    q_send,
    q_recv,
    o_send,
    o_recv,
    s_send,
    s_recv,
):
    half = chips // 2
    group = lax.axis_index("group")
    me = lax.axis_index("blk")
    core = lax.rem(me, CORES)
    other = 1 - core
    chip = lax.div(me, CORES)
    shard = k_in.shape[1]
    local_rows = q_in.shape[1]
    rows_half = local_rows * heads
    columns = CORES * rows_half

    def device(z, on):
        return (group, lax.rem(z + chips, chips) * CORES + on)

    partner = device(chip, other)

    fetch = pltpu.make_async_copy(q_in, q_raw, local_sem.at[0])
    fetch.start()
    barrier = pltpu.get_barrier_semaphore()
    pl.semaphore_signal(barrier, inc=1, device_id=partner, device_id_type=MESH)
    peers = sorted(set(gather_strides + home_strides))
    for stride in peers:
        for way in (-1, 1):
            for on in (0, 1):
                pl.semaphore_signal(
                    barrier, inc=1, device_id=device(chip + way * stride, on), device_id_type=MESH
                )
    my_rows = pl.ds(pl.multiple_of(core * shard, 256), shard)
    my_half = pl.ds(pl.multiple_of(core * rows_half, 64), rows_half)
    locals_ = [
        pltpu.make_async_copy(v_in.at[core], values.at[my_rows], local_sem.at[1]),
        pltpu.make_async_copy(k_in.at[core], keys.at[my_rows], local_sem.at[2]),
        pltpu.make_async_copy(v_in.at[other], v_stage, local_sem.at[3]),
        pltpu.make_async_copy(k_in.at[other], k_stage, local_sem.at[4]),
    ]
    for copy in locals_:
        copy.start()
    fetch.wait()
    for micro in (0, 1):
        flat = q_raw[micro].astype(jnp.float32)
        for head in range(heads):
            wide[micro, pl.ds(head, local_rows, stride=heads)] = flat[
                :, head * HEAD_DIM : (head + 1) * HEAD_DIM
            ]
        packed[micro] = wide[micro].astype(jnp.bfloat16)
    q_all[1, half, my_half] = packed[core]
    pl.semaphore_wait(barrier, 1 + 4 * len(peers))

    def to_partner(src, dst, index):
        return pltpu.make_async_remote_copy(
            src_ref=src,
            dst_ref=dst,
            send_sem=pair_send.at[index],
            recv_sem=pair_recv.at[index],
            device_id=partner,
            device_id_type=MESH,
        )

    def first(way, place, slot, on):
        return pltpu.make_async_remote_copy(
            src_ref=packed.at[on],
            dst_ref=q_all.at[way, slot, my_half],
            send_sem=first_send.at[way, place, on],
            recv_sem=q_recv.at[way, slot],
            device_id=device(chip + (1 - 2 * way) * slot, on),
            device_id_type=MESH,
        )

    firsts = [
        first(way, place, slot, on)
        for place, slot in enumerate(fed_by(0, half, gather_strides))
        for way in (0, 1)
        for on in (0, 1)
    ]
    for copy in firsts:
        copy.start()
    swaps = [
        to_partner(packed.at[other], q_all.at[1, half, my_half], 0),
        to_partner(v_stage, values.at[my_rows], 1),
        to_partner(k_stage, keys.at[my_rows], 2),
    ]
    locals_[2].wait()
    locals_[3].wait()
    for copy in swaps:
        copy.start()

    row = lax.broadcasted_iota(jnp.int32, (columns, HEAD_DIM), 0)
    low = (lax.rem(row, heads) < heads // KV_HEADS).astype(jnp.float32)
    pick[0] = low.astype(jnp.bfloat16)
    pick[1] = (1.0 - low).astype(jnp.bfloat16)

    def relay(way, k, slot, src):
        return pltpu.make_async_remote_copy(
            src_ref=src,
            dst_ref=q_all.at[way, slot],
            send_sem=q_send.at[way, slot],
            recv_sem=q_recv.at[way, slot],
            device_id=device(chip + (1 - 2 * way) * (slot - k), core),
            device_id_type=MESH,
        )

    def arrival(way, k):
        return pltpu.make_async_remote_copy(
            src_ref=q_all.at[way, k],
            dst_ref=q_all.at[way, k],
            send_sem=q_send.at[way, k],
            recv_sem=q_recv.at[way, k],
            device_id=partner,
            device_id_type=MESH,
        )

    length = lengths[core]
    offset = offsets[core]
    base = chip * CORES * shard
    column = lax.broadcasted_iota(jnp.int32, (1, columns), 1)
    head_low = lax.rem(column, heads) < heads // KV_HEADS

    def limit_of(source):
        position = offset + source * (columns // heads) + lax.div(column, heads)
        return jnp.minimum(position + 1, length) - base

    def pieces(k):
        return PIECES if k % home_strides[0] == 0 else 1

    def homeward(way, k, stride, count):
        target = device(chip - (1 - 2 * way) * stride, core)
        copies = [
            pltpu.make_async_remote_copy(
                src_ref=stat.at[way, k, pl.ds(0, 2)],
                dst_ref=got_stat.at[way, k, pl.ds(0, 2)],
                send_sem=s_send.at[way, k],
                recv_sem=s_recv.at[way, k],
                device_id=target,
                device_id_type=MESH,
            )
        ]
        size = HEAD_DIM // count
        for piece in range(count):
            span = pl.ds(piece * size, size)
            copies.append(
                pltpu.make_async_remote_copy(
                    src_ref=send.at[way, k, span],
                    dst_ref=got.at[way, k, span],
                    send_sem=o_send.at[way, k, piece],
                    recv_sem=o_recv.at[way, k, piece],
                    device_id=target,
                    device_id_type=MESH,
                )
            )
        return copies

    def own(way, k):
        return part[way, k], stat[way, k, 0:1], stat[way, k, 1:2]

    def received(way, k):
        for copy in homeward(way, k, 1, pieces(k)):
            copy.wait_recv()
        return got[way, k], got_stat[way, k, 0:1], got_stat[way, k, 1:2]

    def keep(way, k, state):
        part[way, k] = state[0]
        stat[way, k, 0:1] = state[1]
        stat[way, k, 1:2] = state[2]

    def gather(way, k):
        nearby = [c for c in fed_by(k, half - way, home_strides) if c - k < home_strides[0]]
        keep(way, k, merge([own(way, k)] + [received(way, c) for c in nearby]))

    def forward(way, k):
        stride = step_of(k, home_strides)
        far = k + home_strides[0]
        copies = homeward(way, k, stride, pieces(k))
        if stride == home_strides[0] and far <= half - way:
            coming = homeward(way, far, 1, PIECES)
            coming[0].wait_recv()
            best = jnp.maximum(stat[way, k, 0:1], got_stat[way, far, 0:1])
            mine = jnp.exp2((stat[way, k, 0:1] - best) * EXP_SCALE)
            theirs = jnp.exp2((got_stat[way, far, 0:1] - best) * EXP_SCALE)
            stat[way, k, 0:1] = best
            stat[way, k, 1:2] = stat[way, k, 1:2] * mine + got_stat[way, far, 1:2] * theirs
            size = HEAD_DIM // PIECES
            for piece in range(PIECES):
                span = slice(piece * size, (piece + 1) * size)
                coming[1 + piece].wait_recv()
                joined = part[way, k, span] * mine + got[way, far, span] * theirs
                send[way, k, span] = joined.astype(jnp.bfloat16)
                if piece == 0:
                    copies[0].start()
                copies[1 + piece].start()
        else:
            send[way, k] = part[way, k].astype(jnp.bfloat16)
            for copy in copies:
                copy.start()

    def ways(k):
        return [way for way in (0, 1) if k <= half - way]

    def await_block(way, k):
        arrival(way, k).wait_recv()

    top = gather_strides[0]
    near = half - top

    def chunk_at(turn):
        return jnp.where(turn < near, turn + 1, half + near - turn)

    def relay_group(start):
        k = start + top
        for way in ways(k):
            await_block(way, k)
            if k + top <= half - way:
                relay(way, k, k + top, q_all.at[way, k]).start()
        for slot in fed_by(k, half, gather_strides)[1:]:
            for way in ways(slot):
                relay(way, k, slot, q_all.at[way, k]).start()
        for way in (0, 1):
            await_block(way, start + 2)
            relay(way, start + 2, start + 3, q_all.at[way, start + 2]).start()
        for way in (0, 1):
            await_block(way, start + 1)

    scores[...] = jnp.zeros(scores.shape, scores.dtype)
    relay_group(0)
    locals_[0].wait()
    swaps[1].wait()
    for tile in range(values.shape[0] // TILE):
        here = slice(tile * TILE, (tile + 1) * TILE)
        values_t[:, here] = values[here, :].T
    locals_[1].wait()
    swaps[2].wait()
    swaps[0].wait()
    def visit(turn, last_best):
        for start in range(0, half, top):
            if start:
                pl.when(turn == start)(functools.partial(relay_group, start))

            @pl.when(turn == (start + 1 if start == near else start + 2))
            def _(start=start):
                for way in (0, 1):
                    await_block(way, start + 3)

        k = chunk_at(jnp.minimum(turn, half - 1))
        rows = jnp.concatenate([q_all[0, k], q_all[1, k]], axis=0)
        mask = jnp.concatenate([pick[...], pick[...]], axis=1)
        rows = jnp.concatenate([rows * mask[0], rows * mask[1]], axis=1)
        back = lax.select(k == half, 0, k)
        limit = jnp.concatenate(
            [
                limit_of(lax.rem(chip - k + chips, chips)),
                limit_of(lax.rem(chip + back, chips)),
            ],
            axis=1,
        )
        best, numer, total = attend(keys, values_t, scores, rows, limit, last_best)
        done = chunk_at(jnp.maximum(turn - 1, 0))
        for way in (0, 1):
            here = slice(way * columns, (way + 1) * columns)
            mine = jnp.where(head_low, numer[:HEAD_DIM, here], numer[HEAD_DIM:, here])
            keep(way, done, (mine, last_best[:, here], total[:, here]))
            send[way, done] = mine.astype(jnp.bfloat16)

        @pl.when((lax.rem(done, 2) == 1) & (turn > 0))
        def _():
            for way in (0, 1):
                for copy in homeward(way, done, 1, 1):
                    copy.start()

        @pl.when(turn == near + 1)
        def _():
            forward(0, half)

        for start in range(0, near, top):

            @pl.when(turn == start + top + 2)
            def _(start=start):
                for way in (0, 1):
                    gather(way, start + 2)
                    forward(way, start + 2)

        return best

    lax.fori_loop(0, half + 1, visit, jnp.zeros((1, 2 * columns), jnp.float32))

    for way in (0, 1):
        gather(way, near + 2)
        forward(way, near + 2)
    order = sorted(range(top, half, top), key=lambda k: (step_of(k, home_strides), -k))
    for k in order:
        for way in (0, 1):
            gather(way, k)
            forward(way, k)
    state = merge(
        [own(1, half)]
        + [
            received(way, s)
            for s in fed_by(0, half, home_strides)
            if s < home_strides[0]
            for way in (0, 1)
        ]
    )
    state = merge([state] + [received(way, home_strides[0]) for way in (0, 1)])
    merged = (state[0] / state[2]).T
    home[...] = merged.astype(jnp.bfloat16)
    their_half = pl.ds(pl.multiple_of(other * rows_half, 64), rows_half)
    back = to_partner(home.at[their_half], home_got, 3)
    back.start()

    def unpack(micro, rows):
        wide[0] = rows.astype(jnp.float32)
        for head in range(heads):
            out[micro, :, head * HEAD_DIM : (head + 1) * HEAD_DIM] = wide[
                0, pl.ds(head, local_rows, stride=heads)
            ].astype(jnp.bfloat16)

    unpack(core, home[my_half])
    for copy in firsts:
        copy.wait_send()
    for way in (0, 1):
        for k in range(1, half + 1 - way):
            if k not in fed_by(0, half, gather_strides):
                arrival(way, k).wait_send()
            for copy in homeward(way, k, 1, pieces(k)):
                copy.wait_send()
    back.wait()
    unpack(other, home_got[...])


def body(queries, keys, values, lengths, offsets):
    micro, local_rows, row_width = queries.shape
    shard, kv_width = keys.shape[1:]
    heads = row_width // HEAD_DIM
    chips = lax.axis_size("blk") // CORES
    half = chips // 2
    rows_half = local_rows * heads
    columns = CORES * rows_half
    slots = (2, half + 1)
    dma = pltpu.SemaphoreType.DMA
    return pl.pallas_call(
        functools.partial(kernel, chips, heads, (4, 2, 1), (4, 2, 1)),
        out_shape=jax.ShapeDtypeStruct(queries.shape, jnp.bfloat16),
        in_specs=[
            pl.BlockSpec(memory_space=pltpu.SMEM),
            pl.BlockSpec(memory_space=pltpu.SMEM),
            pl.BlockSpec(memory_space=pl.ANY),
            pl.BlockSpec(memory_space=pl.ANY),
            pl.BlockSpec(memory_space=pl.ANY),
        ],
        out_specs=pl.BlockSpec(memory_space=pltpu.VMEM),
        scratch_shapes=[
            pltpu.VMEM((CORES * shard, kv_width), jnp.bfloat16),
            pltpu.VMEM((CORES * shard, kv_width), jnp.bfloat16),
            pltpu.VMEM((kv_width, CORES * shard), jnp.bfloat16),
            pltpu.VMEM((CORES * shard, 2 * columns), jnp.float32),
            pltpu.VMEM((2, columns, HEAD_DIM), jnp.bfloat16),
            pltpu.VMEM((shard, kv_width), jnp.bfloat16),
            pltpu.VMEM((shard, kv_width), jnp.bfloat16),
            pltpu.VMEM(queries.shape, jnp.bfloat16),
            pltpu.VMEM((micro, rows_half, HEAD_DIM), jnp.float32),
            pltpu.VMEM((micro, rows_half, HEAD_DIM), jnp.bfloat16),
            pltpu.VMEM(slots + (columns, HEAD_DIM), jnp.bfloat16),
            pltpu.VMEM(slots + (HEAD_DIM, columns), jnp.float32),
            pltpu.VMEM(slots + (8, columns), jnp.float32),
            pltpu.VMEM(slots + (HEAD_DIM, columns), jnp.bfloat16),
            pltpu.VMEM(slots + (HEAD_DIM, columns), jnp.bfloat16),
            pltpu.VMEM(slots + (8, columns), jnp.float32),
            pltpu.VMEM((columns, HEAD_DIM), jnp.bfloat16),
            pltpu.VMEM((rows_half, HEAD_DIM), jnp.bfloat16),
            dma((5,)),
            dma((4,)),
            dma((4,)),
            dma((2, 3, CORES)),
            dma(slots),
            dma(slots),
            dma(slots + (PIECES,)),
            dma(slots + (PIECES,)),
            dma(slots),
            dma(slots),
        ],
        compiler_params=pltpu.CompilerParams(
            collective_id=0, has_side_effects=True, vmem_limit_bytes=63 * 2**20
        ),
        name="attend_all",
    )(lengths, offsets, queries, keys, values)


def solution(mesh):
    return jax.shard_map(
        body,
        mesh=mesh,
        in_specs=(
            P("group", "blk", None),
            P("group", "blk", None),
            P("group", "blk", None),
            P("group"),
            P("group"),
        ),
        out_specs=P("group", "blk", None),
        check_vma=False,
    )
```

```python
import functools
import math

import jax
import jax.numpy as jnp
from jax import lax
from jax.experimental import pallas as pl
from jax.experimental.pallas import tpu as pltpu
from jax.sharding import PartitionSpec as P

KV_HEADS = 2
HEAD_DIM = 128
CORES = 2
MESH = pl.DeviceIdType.MESH
EXP_SCALE = math.log2(math.e) / math.sqrt(HEAD_DIM)
LOW = -1e30
TILE = 256
PIECES = 1


def step_of(distance, strides):
    return next(stride for stride in strides if distance % stride == 0)


def fed_by(distance, furthest, strides):
    return [
        distance + stride
        for stride in strides
        if distance + stride <= furthest and step_of(distance + stride, strides) == stride
    ]


def merge(parts):
    best = functools.reduce(jnp.maximum, [part[1] for part in parts])
    scales = [jnp.exp2((part[1] - best) * EXP_SCALE) for part in parts]
    numer = sum(part[0].astype(jnp.float32) * scale for part, scale in zip(parts, scales))
    total = sum(part[2] * scale for part, scale in zip(parts, scales))
    return numer, best, total


def attend(keys, values_t, scores_ref, rows, limit, last_best):
    width = rows.shape[0]
    position = lax.broadcasted_iota(jnp.int32, (TILE, width), 0)
    columns = rows.astype(jnp.float32).T.astype(jnp.bfloat16)
    best = numer = total = None
    for tile in range(keys.shape[0] // TILE):
        here = slice(tile * TILE, (tile + 1) * TILE)
        last = scores_ref[here, :]
        scores = jnp.dot(keys[here, :], columns, preferred_element_type=jnp.float32)
        scores = jnp.where(position < limit - tile * TILE, scores, LOW)
        largest = scores.reshape(TILE // 8, 8, width).max(0)
        best = largest if best is None else jnp.maximum(best, largest)
        weights = jnp.exp2((last - last_best) * EXP_SCALE)
        scores_ref[here, :] = scores
        sums = weights.reshape(TILE // 8, 8, width).sum(0)
        total = sums if total is None else total + sums
        product = jnp.dot(
            values_t[:, here], weights.astype(jnp.bfloat16), preferred_element_type=jnp.float32
        )
        numer = product if numer is None else numer + product
    return best.max(0, keepdims=True), numer, total.sum(0, keepdims=True)


def kernel(
    chips,
    heads,
    gather_strides,
    home_strides,
    lengths,
    offsets,
    q_in,
    k_in,
    v_in,
    out,
    keys,
    values,
    values_t,
    scores,
    pick,
    k_stage,
    v_stage,
    q_raw,
    out_raw,
    wide,
    packed,
    q_all,
    part,
    stat,
    send,
    got,
    got_stat,
    home,
    home_got,
    local_sem,
    pair_send,
    pair_recv,
    first_send,
    q_send,
    q_recv,
    o_send,
    o_recv,
    s_send,
    s_recv,
):
    half = chips // 2
    group = lax.axis_index("group")
    me = lax.axis_index("blk")
    core = lax.rem(me, CORES)
    other = 1 - core
    chip = lax.div(me, CORES)
    shard = k_in.shape[1]
    local_rows = q_in.shape[1]
    rows_half = local_rows * heads
    columns = CORES * rows_half

    def device(z, on):
        return (group, lax.rem(z + chips, chips) * CORES + on)

    partner = device(chip, other)

    fetch = pltpu.make_async_copy(q_in, q_raw.at[pl.ds(0, CORES)], local_sem.at[0])
    fetch.start()
    barrier = pltpu.get_barrier_semaphore()
    pl.semaphore_signal(barrier, inc=1, device_id=partner, device_id_type=MESH)
    peers = sorted(set(gather_strides + home_strides))
    for stride in peers:
        for way in (-1, 1):
            for on in (0, 1):
                pl.semaphore_signal(
                    barrier, inc=1, device_id=device(chip + way * stride, on), device_id_type=MESH
                )
    my_rows = pl.ds(pl.multiple_of(core * shard, 256), shard)
    my_half = pl.ds(pl.multiple_of(core * rows_half, 64), rows_half)
    locals_ = [
        pltpu.make_async_copy(v_in.at[core], values.at[my_rows], local_sem.at[1]),
        pltpu.make_async_copy(k_in.at[core], keys.at[my_rows], local_sem.at[2]),
        pltpu.make_async_copy(v_in.at[other], v_stage, local_sem.at[3]),
        pltpu.make_async_copy(k_in.at[other], k_stage, local_sem.at[4]),
    ]
    for copy in locals_:
        copy.start()
    fetch.wait()
    for micro in (0, 1):
        flat = q_raw[micro].astype(jnp.float32)
        for head in range(heads):
            wide[micro, pl.ds(head, local_rows, stride=heads)] = flat[
                :, head * HEAD_DIM : (head + 1) * HEAD_DIM
            ]
        packed[micro] = wide[micro].astype(jnp.bfloat16)
    q_all[1, half, my_half] = packed[core]
    pl.semaphore_wait(barrier, 1 + 4 * len(peers))

    def to_partner(src, dst, index):
        return pltpu.make_async_remote_copy(
            src_ref=src,
            dst_ref=dst,
            send_sem=pair_send.at[index],
            recv_sem=pair_recv.at[index],
            device_id=partner,
            device_id_type=MESH,
        )

    def first(way, place, slot, on):
        return pltpu.make_async_remote_copy(
            src_ref=packed.at[on],
            dst_ref=q_all.at[way, slot, my_half],
            send_sem=first_send.at[way, place, on],
            recv_sem=q_recv.at[way, slot],
            device_id=device(chip + (1 - 2 * way) * slot, on),
            device_id_type=MESH,
        )

    firsts = [
        first(way, place, slot, on)
        for place, slot in enumerate(fed_by(0, half, gather_strides))
        for way in (0, 1)
        for on in (0, 1)
    ]
    for copy in firsts:
        copy.start()
    swaps = [
        to_partner(packed.at[other], q_all.at[1, half, my_half], 0),
        to_partner(v_stage, values.at[my_rows], 1),
        to_partner(k_stage, keys.at[my_rows], 2),
    ]
    locals_[2].wait()
    locals_[3].wait()
    for copy in swaps:
        copy.start()

    row = lax.broadcasted_iota(jnp.int32, (columns, HEAD_DIM), 0)
    low = (lax.rem(row, heads) < heads // KV_HEADS).astype(jnp.float32)
    pick[0] = low.astype(jnp.bfloat16)
    pick[1] = (1.0 - low).astype(jnp.bfloat16)

    def relay(way, k, slot, src):
        return pltpu.make_async_remote_copy(
            src_ref=src,
            dst_ref=q_all.at[way, slot],
            send_sem=q_send.at[way, slot],
            recv_sem=q_recv.at[way, slot],
            device_id=device(chip + (1 - 2 * way) * (slot - k), core),
            device_id_type=MESH,
        )

    def arrival(way, k):
        return pltpu.make_async_remote_copy(
            src_ref=q_all.at[way, k],
            dst_ref=q_all.at[way, k],
            send_sem=q_send.at[way, k],
            recv_sem=q_recv.at[way, k],
            device_id=partner,
            device_id_type=MESH,
        )

    length = lengths[core]
    offset = offsets[core]
    base = chip * CORES * shard
    column = lax.broadcasted_iota(jnp.int32, (1, columns), 1)
    head_low = lax.rem(column, heads) < heads // KV_HEADS

    def limit_of(source):
        position = offset + source * (columns // heads) + lax.div(column, heads)
        return jnp.minimum(position + 1, length) - base

    def pieces(k):
        return PIECES if k % home_strides[0] == 0 else 1

    def homeward(way, k, stride, count):
        target = device(chip - (1 - 2 * way) * stride, core)
        copies = [
            pltpu.make_async_remote_copy(
                src_ref=stat.at[way, k, pl.ds(0, 2)],
                dst_ref=got_stat.at[way, k, pl.ds(0, 2)],
                send_sem=s_send.at[way, k],
                recv_sem=s_recv.at[way, k],
                device_id=target,
                device_id_type=MESH,
            )
        ]
        size = HEAD_DIM // count
        for piece in range(count):
            span = pl.ds(piece * size, size)
            copies.append(
                pltpu.make_async_remote_copy(
                    src_ref=send.at[way, k, span],
                    dst_ref=got.at[way, k, span],
                    send_sem=o_send.at[way, k, piece],
                    recv_sem=o_recv.at[way, k, piece],
                    device_id=target,
                    device_id_type=MESH,
                )
            )
        return copies

    def own(way, k):
        return part[way, k], stat[way, k, 0:1], stat[way, k, 1:2]

    def received(way, k):
        for copy in homeward(way, k, 1, pieces(k)):
            copy.wait_recv()
        return got[way, k], got_stat[way, k, 0:1], got_stat[way, k, 1:2]

    def keep(way, k, state):
        part[way, k] = state[0]
        stat[way, k, 0:1] = state[1]
        stat[way, k, 1:2] = state[2]

    def gather(way, k):
        nearby = [c for c in fed_by(k, half - way, home_strides) if c - k < home_strides[0]]
        keep(way, k, merge([own(way, k)] + [received(way, c) for c in nearby]))

    def forward(way, k):
        stride = step_of(k, home_strides)
        far = k + home_strides[0]
        copies = homeward(way, k, stride, pieces(k))
        if stride == home_strides[0] and far <= half - way:
            coming = homeward(way, far, 1, PIECES)
            coming[0].wait_recv()
            best = jnp.maximum(stat[way, k, 0:1], got_stat[way, far, 0:1])
            mine = jnp.exp2((stat[way, k, 0:1] - best) * EXP_SCALE)
            theirs = jnp.exp2((got_stat[way, far, 0:1] - best) * EXP_SCALE)
            stat[way, k, 0:1] = best
            stat[way, k, 1:2] = stat[way, k, 1:2] * mine + got_stat[way, far, 1:2] * theirs
            size = HEAD_DIM // PIECES
            for piece in range(PIECES):
                span = slice(piece * size, (piece + 1) * size)
                coming[1 + piece].wait_recv()
                joined = part[way, k, span] * mine + got[way, far, span] * theirs
                send[way, k, span] = joined.astype(jnp.bfloat16)
                if piece == 0:
                    copies[0].start()
                copies[1 + piece].start()
        else:
            send[way, k] = part[way, k].astype(jnp.bfloat16)
            for copy in copies:
                copy.start()

    def ways(k):
        return [way for way in (0, 1) if k <= half - way]

    def await_block(way, k):
        arrival(way, k).wait_recv()

    top = gather_strides[0]
    near = half - top

    def chunk_at(turn):
        return jnp.where(turn < near, turn + 1, half + near - turn)

    def relay_group(start):
        k = start + top
        for way in ways(k):
            await_block(way, k)
            if k + top <= half - way:
                relay(way, k, k + top, q_all.at[way, k]).start()
        for slot in fed_by(k, half, gather_strides)[1:]:
            for way in ways(slot):
                relay(way, k, slot, q_all.at[way, k]).start()
        for way in (0, 1):
            await_block(way, start + 2)
            relay(way, start + 2, start + 3, q_all.at[way, start + 2]).start()
        for way in (0, 1):
            await_block(way, start + 1)

    scores[...] = jnp.zeros(scores.shape, scores.dtype)
    relay_group(0)
    locals_[0].wait()
    swaps[1].wait()
    for tile in range(values.shape[0] // TILE):
        here = slice(tile * TILE, (tile + 1) * TILE)
        values_t[:, here] = values[here, :].T
    locals_[1].wait()
    swaps[2].wait()
    swaps[0].wait()
    def visit(turn, last_best):
        for start in range(0, half, top):
            if start:
                pl.when(turn == start)(functools.partial(relay_group, start))

            @pl.when(turn == (start + 1 if start == near else start + 2))
            def _(start=start):
                for way in (0, 1):
                    await_block(way, start + 3)

        k = chunk_at(jnp.minimum(turn, half - 1))
        rows = jnp.concatenate([q_all[0, k], q_all[1, k]], axis=0)
        mask = jnp.concatenate([pick[...], pick[...]], axis=1)
        rows = jnp.concatenate([rows * mask[0], rows * mask[1]], axis=1)
        back = lax.select(k == half, 0, k)
        limit = jnp.concatenate(
            [
                limit_of(lax.rem(chip - k + chips, chips)),
                limit_of(lax.rem(chip + back, chips)),
            ],
            axis=1,
        )
        best, numer, total = attend(keys, values_t, scores, rows, limit, last_best)
        done = chunk_at(jnp.maximum(turn - 1, 0))
        for way in (0, 1):
            here = slice(way * columns, (way + 1) * columns)
            mine = jnp.where(head_low, numer[:HEAD_DIM, here], numer[HEAD_DIM:, here])
            keep(way, done, (mine, last_best[:, here], total[:, here]))
            send[way, done] = mine.astype(jnp.bfloat16)

        @pl.when((lax.rem(done, 2) == 1) & (turn > 0))
        def _():
            for way in (0, 1):
                for copy in homeward(way, done, 1, 1):
                    copy.start()

        @pl.when(turn == near + 1)
        def _():
            forward(0, half)

        for start in range(0, near, top):

            @pl.when(turn == start + top + 2)
            def _(start=start):
                for way in (0, 1):
                    gather(way, start + 2)
                    forward(way, start + 2)

        return best

    lax.fori_loop(0, half + 1, visit, jnp.zeros((1, 2 * columns), jnp.float32))

    for way in (0, 1):
        gather(way, near + 2)
        forward(way, near + 2)
    order = sorted(range(top, half, top), key=lambda k: (step_of(k, home_strides), -k))
    for k in order:
        for way in (0, 1):
            gather(way, k)
            forward(way, k)
    state = merge(
        [own(1, half)]
        + [
            received(way, s)
            for s in fed_by(0, half, home_strides)
            if s < home_strides[0]
            for way in (0, 1)
        ]
    )
    state = merge([state] + [received(way, home_strides[0]) for way in (0, 1)])
    merged = (state[0] / state[2]).T
    home[...] = merged.astype(jnp.bfloat16)
    their_half = pl.ds(pl.multiple_of(other * rows_half, 64), rows_half)
    back = to_partner(home.at[their_half], home_got, 3)
    back.start()

    def unpack(micro, rows):
        wide[0] = rows.astype(jnp.float32)
        for head in range(heads):
            out_raw[micro, :, head * HEAD_DIM : (head + 1) * HEAD_DIM] = wide[
                0, pl.ds(head, local_rows, stride=heads)
            ].astype(jnp.bfloat16)

    unpack(core, home[my_half])
    for copy in firsts:
        copy.wait_send()
    for way in (0, 1):
        for k in range(1, half + 1 - way):
            if k not in fed_by(0, half, gather_strides):
                arrival(way, k).wait_send()
            for copy in homeward(way, k, 1, pieces(k)):
                copy.wait_send()
    back.wait()
    unpack(other, home_got[...])
    store = pltpu.make_async_copy(out_raw.at[pl.ds(0, CORES)], out, local_sem.at[0])
    store.start()
    store.wait()


def body(queries, keys, values, lengths, offsets):
    micro, local_rows, row_width = queries.shape
    shard, kv_width = keys.shape[1:]
    heads = row_width // HEAD_DIM
    chips = lax.axis_size("blk") // CORES
    half = chips // 2
    rows_half = local_rows * heads
    columns = CORES * rows_half
    slots = (2, half + 1)
    dma = pltpu.SemaphoreType.DMA
    return pl.pallas_call(
        functools.partial(kernel, chips, heads, (4, 2, 1), (4, 2, 1)),
        out_shape=jax.ShapeDtypeStruct(queries.shape, jnp.bfloat16),
        in_specs=[
            pl.BlockSpec(memory_space=pltpu.SMEM),
            pl.BlockSpec(memory_space=pltpu.SMEM),
            pl.BlockSpec(memory_space=pl.ANY),
            pl.BlockSpec(memory_space=pl.ANY),
            pl.BlockSpec(memory_space=pl.ANY),
        ],
        out_specs=pl.BlockSpec(memory_space=pl.ANY),
        scratch_shapes=[
            pltpu.VMEM((CORES * shard, kv_width), jnp.bfloat16),
            pltpu.VMEM((CORES * shard, kv_width), jnp.bfloat16),
            pltpu.VMEM((kv_width, CORES * shard), jnp.bfloat16),
            pltpu.VMEM((CORES * shard, 2 * columns), jnp.float32),
            pltpu.VMEM((2, columns, HEAD_DIM), jnp.bfloat16),
            pltpu.VMEM((shard, kv_width), jnp.bfloat16),
            pltpu.VMEM((shard, kv_width), jnp.bfloat16),
            pltpu.VMEM((micro + 2, local_rows, row_width), jnp.bfloat16),
            pltpu.VMEM((micro + 2, local_rows, row_width), jnp.bfloat16),
            pltpu.VMEM((micro + 2, rows_half, HEAD_DIM), jnp.float32),
            pltpu.VMEM((micro, rows_half, HEAD_DIM), jnp.bfloat16),
            pltpu.VMEM(slots + (columns, HEAD_DIM), jnp.bfloat16),
            pltpu.VMEM(slots + (HEAD_DIM, columns), jnp.float32),
            pltpu.VMEM(slots + (8, columns), jnp.float32),
            pltpu.VMEM(slots + (HEAD_DIM, columns), jnp.bfloat16),
            pltpu.VMEM(slots + (HEAD_DIM, columns), jnp.bfloat16),
            pltpu.VMEM(slots + (8, columns), jnp.float32),
            pltpu.VMEM((columns, HEAD_DIM), jnp.bfloat16),
            pltpu.VMEM((rows_half, HEAD_DIM), jnp.bfloat16),
            dma((5,)),
            dma((4,)),
            dma((4,)),
            dma((2, 3, CORES)),
            dma(slots),
            dma(slots),
            dma(slots + (PIECES,)),
            dma(slots + (PIECES,)),
            dma(slots),
            dma(slots),
        ],
        compiler_params=pltpu.CompilerParams(
            collective_id=0, has_side_effects=True, vmem_limit_bytes=63 * 2**20
        ),
        name="attend_all",
    )(lengths, offsets, queries, keys, values)


def solution(mesh):
    return jax.shard_map(
        body,
        mesh=mesh,
        in_specs=(
            P("group", "blk", None),
            P("group", "blk", None),
            P("group", "blk", None),
            P("group"),
            P("group"),
        ),
        out_specs=P("group", "blk", None),
        check_vma=False,
    )
```
